16 devices in a mesh: data: 16 (over z, y, x, core).
Axes of the slice: x: 2, y: 2, z: 2, core: 2. Of those that a mesh axis runs over, the one named last changes fastest.
Arguments:
- x_in: bfloat16 [192, 128, 1024], P('data')
- g_out: bfloat16 [192, 128, 1024], P('data')
- step_emb: bfloat16 [4, 1024], replicated
- w_q: bfloat16 [1024, 16, 64], replicated
- w_k: bfloat16 [1024, 16, 64], replicated
- w_v: bfloat16 [1024, 16, 64], replicated
- w_o: bfloat16 [16, 64, 1024], replicated
- w_up: bfloat16 [1024, 4096], replicated
- w_down: bfloat16 [4096, 1024], replicated
Outputs:
- output 1: float32 [1024, 16, 64], replicated
- output 2: float32 [1024, 16, 64], replicated
- output 3: float32 [1024, 16, 64], replicated
- output 4: float32 [16, 64, 1024], replicated
- output 5: float32 [1024, 4096], replicated
- output 6: float32 [4096, 1024], replicated
- output 7: bfloat16 [192, 128, 1024], P('data')
All inputs are finite; a program needn't handle non-finite values.
Results may differ from the reference program's by a relative error of at most 0.02.
Values are sent between devices in bfloat16 or wider.
A program may use at most 1 GiB of HBM per device.

```python
import math
import functools
import jax
import jax.numpy as jnp
from jax import lax

D = 1024
FF = 4096
HEADS = 16
SEQ = 128
LAYERS = 4
BATCH = 192
HEAD = D // HEADS
NORM_EPS = 1e-6


def setup_inputs(seed: int = 0) -> dict:
    sub_keys = jax.random.split(jax.random.key(seed), 9)
    out_gain = 2.0 / math.sqrt(LAYERS)
    x_in = jax.random.normal(sub_keys[0], (BATCH, SEQ, D), jnp.float32)
    g_out = jax.random.normal(sub_keys[1], (BATCH, SEQ, D), jnp.float32)
    step_emb = jax.random.normal(sub_keys[2], (LAYERS, D), jnp.float32) / math.sqrt(LAYERS)
    w_q = jax.random.normal(sub_keys[3], (D, HEADS, HEAD), jnp.float32) * D ** -0.5
    w_k = jax.random.normal(sub_keys[4], (D, HEADS, HEAD), jnp.float32) * D ** -0.5
    w_v = jax.random.normal(sub_keys[5], (D, HEADS, HEAD), jnp.float32) * D ** -0.5
    w_o = jax.random.normal(sub_keys[6], (HEADS, HEAD, D), jnp.float32) * (D ** -0.5 * out_gain)
    w_up = jax.random.normal(sub_keys[7], (D, FF), jnp.float32) * D ** -0.5
    w_down = jax.random.normal(sub_keys[8], (FF, D), jnp.float32) * (FF ** -0.5 * out_gain)
    return {
        'x_in': x_in.astype(jnp.bfloat16),
        'g_out': g_out.astype(jnp.bfloat16),
        'step_emb': step_emb.astype(jnp.bfloat16),
        'w_q': w_q.astype(jnp.bfloat16),
        'w_k': w_k.astype(jnp.bfloat16),
        'w_v': w_v.astype(jnp.bfloat16),
        'w_o': w_o.astype(jnp.bfloat16),
        'w_up': w_up.astype(jnp.bfloat16),
        'w_down': w_down.astype(jnp.bfloat16),
    }


def rms_norm(x_val):
    x_f32 = x_val.astype(jnp.float32)
    return (x_f32 * lax.rsqrt(jnp.mean(x_f32 * x_f32, axis=-1, keepdims=True) + NORM_EPS)).astype(jnp.bfloat16)


def shared_block(weight_set, x_prev, step_vec):
    w_q, w_k, w_v, w_o, w_up, w_down = weight_set
    x_cur = x_prev + step_vec
    u_norm = rms_norm(x_cur).astype(jnp.float32)
    q_heads = jnp.einsum('sd,dhe->she', u_norm, w_q).astype(jnp.bfloat16)
    k_heads = jnp.einsum('sd,dhe->she', u_norm, w_k).astype(jnp.bfloat16)
    v_heads = jnp.einsum('sd,dhe->she', u_norm, w_v).astype(jnp.bfloat16)
    scores = jnp.einsum('qhe,khe->hqk', q_heads.astype(jnp.float32), k_heads.astype(jnp.float32)).astype(jnp.bfloat16)
    prob_mat = jax.nn.softmax(scores.astype(jnp.float32) * HEAD ** -0.5, axis=-1).astype(jnp.bfloat16)
    mix_heads = jnp.einsum('hqk,khe->qhe', prob_mat.astype(jnp.float32), v_heads.astype(jnp.float32)).astype(jnp.bfloat16)
    attn_out = jnp.einsum('qhe,hed->qd', mix_heads.astype(jnp.float32), w_o).astype(jnp.bfloat16)
    h_mid = x_cur + attn_out
    m_norm = rms_norm(h_mid).astype(jnp.float32)
    z_up = jnp.dot(m_norm, w_up, preferred_element_type=jnp.float32).astype(jnp.bfloat16)
    g_act = jax.nn.gelu(z_up.astype(jnp.float32), approximate=True).astype(jnp.bfloat16)
    y_down = jnp.dot(g_act.astype(jnp.float32), w_down, preferred_element_type=jnp.float32).astype(jnp.bfloat16)
    return h_mid + y_down


def run_stack(weight_set, x_seq, step_emb):
    def layer_step(x_cur, step_vec):
        return jax.checkpoint(shared_block)(weight_set, x_cur, step_vec), None
    x_out, unused = lax.scan(layer_step, x_seq, step_emb)
    return x_out


def reference(x_in, g_out, step_emb, w_q, w_k, w_v, w_o, w_up, w_down):
    weight_set = tuple(w.astype(jnp.float32) for w in (w_q, w_k, w_v, w_o, w_up, w_down))

    def seq_grads(grad_acc, seq_pair):
        x_seq, g_seq = seq_pair
        x_out, pull_back = jax.vjp(functools.partial(run_stack, step_emb=step_emb), weight_set, x_seq)
        d_weights, d_x = pull_back(g_seq)
        return tuple(a + b for a, b in zip(grad_acc, d_weights)), d_x

    zero_acc = tuple(jnp.zeros_like(w) for w in weight_set)
    grad_sums, grad_x = lax.scan(seq_grads, zero_acc, (x_in, g_out))
    return (grad_sums[0], grad_sums[1], grad_sums[2], grad_sums[3], grad_sums[4], grad_sums[5], grad_x)
```

```python
import functools
import itertools
import math
import jax, jax.numpy as jnp
from jax import lax
from jax.sharding import PartitionSpec as P
from jax.experimental import pallas as pl
from jax.experimental.pallas import tpu as pltpu

BF, F32 = jnp.bfloat16, jnp.float32
EPS = 1e-6
VLIM = 67_043_328
LANE = 128
DEVS, BLOCKS, PARTS, NSUB = 16, 8, 4, 4
SERVE = (((1, 3),), ((3, 6),), ((0, 1), (2, 4)), ())
ABUF = ("sbuf", "dbuf", "pbuf", "gbuf")
C_GELU = math.sqrt(2.0 / math.pi)


def dot(a, b, ca=1, cb=0):
    return lax.dot_general(a, b, (((ca,), (cb,)), ((), ())), preferred_element_type=F32)


def rms(xf):
    r = lax.rsqrt(jnp.mean(xf * xf, axis=-1, keepdims=True) + EPS)
    return (xf * r).astype(BF)


def gelu(z):
    zf = z.astype(F32)
    t = jnp.tanh(C_GELU * (zf + 0.044715 * (zf * zf * zf)))
    return (zf * (0.5 * (1.0 + t))).astype(BF)


def pair_cat(x, lo, hi):
    return jnp.concatenate([x * lo, x * hi], axis=0)


def halves(x):
    return jnp.concatenate([x[:, :LANE], x[:, LANE:]], axis=0)


def qkv_of(ref, item, hw):
    r, c = item
    return (ref[r:r + LANE, i * hw + c:i * hw + c + LANE] for i in range(3))


def pair_groups(R, hw, group):
    items = [(r, c) for r in range(0, R, LANE) for c in range(0, hw, LANE)]
    return [items[i:i + group] for i in range(0, len(items), group)]


def staged(groups, stages):
    n, m = len(groups), len(stages)
    for t in range(n + m - 1):
        for s in reversed(range(m)):
            if 0 <= t - s < n:
                for j, item in enumerate(groups[t - s]):
                    stages[s](item, (t - s) % 2, j)


def softmax_t(st, c2):
    mx = jnp.max(st, axis=0, keepdims=True)
    e = jnp.exp2((st - mx) * c2)
    return e * (1.0 / jnp.sum(e, axis=0, keepdims=True))


def attn_fwd(qkv, mix, R, hw, group, sbuf, pbuf, masks, c2):
    def scores(item, slot, j):
        q, k, _ = qkv_of(qkv, item, hw)
        sbuf[slot, j] = dot(k, pair_cat(q, *masks), 1, 1).astype(BF)

    def probs(item, slot, j):
        pbuf[slot, j] = softmax_t(sbuf[slot, j].astype(F32), c2).astype(BF)

    def mixing(item, slot, j):
        r, c = item
        v = qkv[r:r + LANE, 2 * hw + c:2 * hw + c + LANE]
        mix[r:r + LANE, c:c + LANE] = dot(halves(pbuf[slot, j]), pair_cat(v, *masks), 0, 0).astype(BF)
    staged(pair_groups(R, hw, group), (scores, probs, mixing))


def head_masks():
    lane = lax.broadcasted_iota(jnp.int32, (1, LANE), 1)
    return tuple(m.astype(F32).astype(BF) for m in (lane < LANE // 2, lane >= LANE // 2))


def for_rows(R, chunk, body):
    for r in range(0, R, chunk):
        body(slice(r, r + chunk))


def for_tiles(n, w, body):
    for c in range(0, n, w):
        body(slice(c, c + w))


def qkv_copies(hs, dst, sem, base):
    n = hs[0].shape[0]
    return [pltpu.make_async_copy(h, dst.at[pl.ds(i * n, n)], sem.at[base + i]) for i, h in enumerate(hs)]


def fwd_kernel(cfg, x_hbm, emb_ref, wq_h, wk_h, wv_h, wo_h, wup_h, wdown_h,
               xs_h, us_h, qkv_h, mix_h, hs_h, ms_h, z_h, g_h,
               wqkv, wo, wup, wdown, xin, xs, us, qkv, mix, hs, ms, z, g, sbuf, pbuf, wsem, xsem, osem):
    R, NL, c2, upt, pu = cfg["R"], cfg["L"], cfg["c2"], cfg["upt"], cfg["pu"]
    D, FF, QW = wo.shape[1], wup.shape[1], wo.shape[0]
    b = pl.program_id(0)
    nb = pl.num_programs(0)
    wcopies = qkv_copies((wq_h, wk_h, wv_h), wqkv, wsem, 0) + [pltpu.make_async_copy(h, v, wsem.at[3 + i]) for i, (h, v) in enumerate(((wo_h, wo), (wup_h, wup), (wdown_h, wdown)))]
    row = pl.multiple_of(b * R, R)

    @pl.when(b == 0)
    def _():
        pltpu.make_async_copy(x_hbm.at[pl.ds(0, R)], xin, xsem).start()
        for c in wcopies:
            c.start()

    pltpu.make_async_copy(x_hbm.at[pl.ds(0, R)], xin, xsem).wait()
    masks = head_masks()
    outs = [(xs, xs_h), (us, us_h), (qkv, qkv_h), (mix, mix_h), (hs, hs_h), (ms, ms_h), (z, z_h), (g, g_h)]

    def out_copy(i, l):
        return pltpu.make_async_copy(outs[i][0], outs[i][1].at[l, pl.ds(row, R)], osem.at[i])

    def layer(l, carry):
        notfirst = (b > 0) | (l > 0)
        first = jnp.logical_not(notfirst)

        def free(i):
            @pl.when(notfirst)
            def _():
                out_copy(i, 0).wait()

        def wready(i):
            @pl.when(first)
            def _():
                wcopies[i].wait()

        free(0)
        free(1)
        ch = cfg["ch"]

        def enter(rows):
            xc = xin[rows] + emb_ref[l][0:1]
            xs[rows] = xc
            us[rows] = rms(xc.astype(F32))
        for_rows(R, ch, enter)
        out_copy(0, l).start()
        out_copy(1, l).start()
        for i in range(3):
            wready(i)
        free(2)

        def qkv_tile(cs):
            qkv[:, cs] = dot(us[...], wqkv[cs, :], 1, 1).astype(BF)
        for_tiles(wqkv.shape[0], cfg["nq"], qkv_tile)
        out_copy(2, l).start()
        free(3)
        attn_fwd(qkv, mix, R, QW, cfg["pu"], sbuf, pbuf, masks, c2)
        out_copy(3, l).start()
        wready(3)
        free(4)
        free(5)

        def o_tile(cs):
            hs[:, cs] = xs[:, cs] + dot(mix[...], wo[:, cs]).astype(BF)
        for_tiles(D, cfg["no"], o_tile)
        out_copy(4, l).start()

        def norm_h(rows):
            ms[rows] = rms(hs[rows].astype(F32))
        for_rows(R, ch, norm_h)
        out_copy(5, l).start()
        wready(4)
        free(6)
        free(7)

        def up_tile(cs):
            zz = dot(ms[...], wup[:, cs]).astype(BF)
            z[:, cs] = zz
            g[:, cs] = gelu(zz)
        for_tiles(FF, upt, up_tile)
        out_copy(6, l).start()
        out_copy(7, l).start()
        wready(5)

        @pl.when(l < NL - 1)
        def _():
            def down_tile(cs):
                xin[:, cs] = hs[:, cs] + dot(g[...], wdown[:, cs]).astype(BF)
            for_tiles(D, cfg["nd"], down_tile)
        return carry

    lax.fori_loop(0, NL, layer, 0)

    @pl.when(b + 1 < nb)
    def _():
        pltpu.make_async_copy(x_hbm.at[pl.ds(pl.multiple_of((b + 1) * R, R), R)], xin, xsem).start()

    @pl.when(b + 1 == nb)
    def _():
        for i in range(8):
            out_copy(i, 0).wait()


def fwd(x, emb, wq, wk, wv, wo, wup, wdown, R=512, upt=512, pu=4, nq=1024, no=1024, nd=1024, ch=64, lp=None, **kw):
    T, D = x.shape
    L = emb.shape[0]
    FF, QW = wup.shape[1], wo.shape[0]
    cfg = dict(R=R, L=L, c2=(64 ** -0.5) * math.log2(math.e), upt=upt, pu=pu, nq=nq, no=no, nd=nd, ch=ch, **kw)
    any_ = pl.BlockSpec(memory_space=pl.ANY)
    ws = [D, D, 3 * QW, QW, D, D, FF, FF]
    return pl.pallas_call(
        functools.partial(fwd_kernel, cfg),
        grid=(T // R,),
        out_shape=[jax.ShapeDtypeStruct((L, T, w), BF) for w in ws],
        in_specs=[any_, pl.BlockSpec((L, 16, D), lambda b: (0, 0, 0))] + [any_] * 6,
        out_specs=[any_] * 8,
        scratch_shapes=[pltpu.VMEM((3 * QW, D), BF)] + [pltpu.VMEM(w.shape, BF) for w in (wo, wup, wdown)] + [pltpu.VMEM((R, D), BF)]
        + [pltpu.VMEM((R, w), BF) for w in ws] + [pltpu.VMEM((2, pu, LANE, 2 * LANE), BF)] * 2 + [pltpu.SemaphoreType.DMA((6,)), pltpu.SemaphoreType.DMA, pltpu.SemaphoreType.DMA((8,))],
        compiler_params=pltpu.CompilerParams(vmem_limit_bytes=VLIM, dimension_semantics=("arbitrary",), flags=lp or {}),
        cost_estimate=pl.CostEstimate(flops=2 * L * T * D * (4 * QW + 2 * FF), bytes_accessed=2 * L * T * sum(ws), transcendentals=0),
        name="fwd_layers",
    )(x, jnp.broadcast_to(emb[:, None], (L, 16, D)), wq, wk, wv, wo, wup, wdown)


def rms_vjp(xb, dy):
    xf = xb.astype(F32)
    dyf = dy.astype(F32)
    r = lax.rsqrt(jnp.mean(xf * xf, axis=-1, keepdims=True) + EPS)
    c = jnp.mean(xf * dyf, axis=-1, keepdims=True) * (r * r * r)
    return (r * dyf - xf * c).astype(BF)


def gelu_grad(z, da):
    zf = z.astype(F32)
    z2 = zf * zf
    t = jnp.tanh(zf * (C_GELU + (C_GELU * 0.044715) * z2))
    d = 0.5 * (1.0 + t) + (0.5 * zf) * (1.0 - t * t) * (C_GELU + (3 * 0.044715 * C_GELU) * z2)
    return (da.astype(F32) * d).astype(BF)


def attn_bwd(qkv, dmix, dqkv, R, hw, group, bufs, masks, c2, scale):
    sbuf, dbuf, pbuf, gbuf = bufs

    def at(i, item):
        r, c = item
        return slice(r, r + LANE), slice(i * hw + c, i * hw + c + LANE)

    def scores(item, slot, j):
        q, k, v = qkv_of(qkv, item, hw)
        sbuf[slot, j] = dot(k, pair_cat(q, *masks), 1, 1).astype(BF)
        dbuf[slot, j] = dot(v, pair_cat(dmix[at(0, item)], *masks), 1, 1).astype(BF)

    def probs(item, slot, j):
        p = softmax_t(sbuf[slot, j].astype(F32), c2)
        pdp = p * dbuf[slot, j].astype(F32)
        pbuf[slot, j] = p.astype(BF)
        gbuf[slot, j] = ((pdp - p * jnp.sum(pdp, axis=0, keepdims=True)) * scale).astype(BF)

    def grads(item, slot, j):
        q, k, _ = qkv_of(qkv, item, hw)
        ds = gbuf[slot, j]
        dqkv[at(2, item)] = dot(pbuf[slot, j], pair_cat(dmix[at(0, item)], *masks)).astype(BF)
        dqkv[at(1, item)] = dot(ds, pair_cat(q, *masks)).astype(BF)
        dqkv[at(0, item)] = dot(halves(ds), pair_cat(k, *masks), 0, 0).astype(BF)
    staged(pair_groups(R, hw, group), (scores, probs, grads))


def bwd_kernel(cfg, *refs):
    R, NL, lo, mlp, att = cfg["R"], cfg["NL"], cfg["lo"], cfg["mlp"], cfg["att"]
    names = cfg["names"]
    r = dict(zip(names, refs))
    b = pl.program_id(0)
    nb = pl.num_programs(0)
    row = pl.multiple_of(b * R, R)
    masks = head_masks()
    wn = cfg["weights"]
    wc = {n: [pltpu.make_async_copy(r[n + "_h"], r[n], r["wsem"].at[i])] for i, n in enumerate(wn) if n != "wqkv"}
    if "wqkv" in wn:
        wc["wqkv"] = qkv_copies([r[n + "_h"] for n in ("wq", "wk", "wv")], r["wqkv"], r["wsem"], 4)
    ins = cfg["ins"]
    outs = cfg["outs"]

    def in_copy(n, bb, l):
        rr = pl.ds(pl.multiple_of(bb * R, R), R)
        return pltpu.make_async_copy(r[n + "_h"].at[l, rr], r[n], r["isem"].at[ins.index(n)])

    def out_copy(n, i):
        return pltpu.make_async_copy(r[n], r[n + "_h"].at[i, pl.ds(row, R)], r["osem"].at[outs.index(n)])

    def din_copy(bb):
        return pltpu.make_async_copy(r["din_h"].at[pl.ds(pl.multiple_of(bb * R, R), R)], r["d"], r["dsem"])

    top = lo + NL - 1

    @pl.when(b == 0)
    def _():
        din_copy(0).start()
        for i, n in enumerate(ins):
            in_copy(n, 0, top).start()
            if i < len(wn):
                for c in wc[wn[i]]:
                    c.start()
        for n in wn[len(ins):]:
            for c in wc[n]:
                c.start()

    din_copy(0).wait()

    def layer(i, carry):
        l = top - i
        notfirst = (b > 0) | (i > 0)
        first = jnp.logical_not(notfirst)
        lastl = i == NL - 1
        nb_ = jnp.where(lastl, b + 1, b)
        nl_ = jnp.where(lastl, top, l - 1)

        def free(n):
            @pl.when(notfirst)
            def _():
                out_copy(n, 0).wait()

        def wready(n):
            @pl.when(first)
            def _():
                for c in wc[n]:
                    c.wait()

        def ready(n):
            in_copy(n, 0, 0).wait()

        def prefetch(n):
            @pl.when(nb_ < nb)
            def _():
                in_copy(n, nb_, nl_).start()

        d, tmp = r["d"], r["tmp"]
        if mlp:
            z, hs, dup, wdown, wup = r["z"], r["hs"], r["dup"], r["wdown"], r["wup"]
            if att:
                free("dout")
                r["dout"][...] = d[...]
                out_copy("dout", NL - 1 - i).start()
            ready("z")
            wready("wdown")
            free("dup")
            ft = cfg["ft"]

            def act_tile(cs):
                da = dot(d[...], wdown[cs, :], 1, 1).astype(BF)
                dup[:, cs] = gelu_grad(z[:, cs], da)
            for_tiles(dup.shape[1], ft, act_tile)
            out_copy("dup", NL - 1 - i).start()
            prefetch("z")
            wready("wup")


            def nh_tile(cs):
                tmp[:, cs] = dot(dup[...], wup[cs, :], 1, 1).astype(BF)
            for_tiles(tmp.shape[1], cfg["nt"], nh_tile)
            ready("hs")
            free("dmid")

            def mid_rows(rows):
                r["dmid"][rows] = d[rows] + rms_vjp(hs[rows], tmp[rows])
            for_rows(R, cfg["ch"], mid_rows)
            prefetch("hs")
            out_copy("dmid", NL - 1 - i).start()
        if att:
            dm = r["dmid"] if mlp else d
            qkv, xs, dqkv, wo, wqkv = r["qkv"], r["xs"], r["dqkv"], r["wo"], r["wqkv"]
            wready("wo")


            def mix_tile(cs):
                tmp[:, cs] = dot(dm[...], wo[cs, :], 1, 1).astype(BF)
            for_tiles(tmp.shape[1], cfg["nt"], mix_tile)
            ready("qkv")
            free("dqkv")
            hw = wo.shape[0]

            attn_bwd(qkv, tmp, dqkv, R, hw, cfg["pu"], [r[n] for n in ABUF], masks, cfg["c2"], cfg["scale"])
            prefetch("qkv")
            out_copy("dqkv", NL - 1 - i).start()
            wready("wqkv")


            def nx_tile(cs):
                tmp[:, cs] = dot(dqkv[...], wqkv[:, cs]).astype(BF)
            for_tiles(tmp.shape[1], cfg["nt"], nx_tile)
            ready("xs")

            def out_rows(rows):
                d[rows] = dm[rows] + rms_vjp(xs[rows], tmp[rows])
            for_rows(R, cfg["ch"], out_rows)
            prefetch("xs")
        return carry

    lax.fori_loop(0, NL, layer, 0)
    if att:
        dfin = pltpu.make_async_copy(r["d"], r["dfin_h"].at[pl.ds(row, R)], r["fsem"])
        dfin.start()
        dfin.wait()

    @pl.when(b + 1 < nb)
    def _():
        din_copy(b + 1).start()

    @pl.when(b + 1 == nb)
    def _():
        for n in outs:
            out_copy(n, 0).wait()


def bwd(din, saved, weights, NL, lo, mlp=True, att=True, R=512, ft=512, pu=4, ch=64, nt=1024, lp=None, **kw):
    T, D = din.shape
    FF = weights["wup"].shape[1] if mlp else 0
    wn = (["wdown", "wup"] if mlp else []) + (["wo", "wqkv"] if att else [])
    wn_h = [m for n in wn for m in (("wq", "wk", "wv") if n == "wqkv" else (n,))]
    ins = (["z", "hs"] if mlp else []) + (["qkv", "xs"] if att else [])
    outs = (["dout"] if mlp and att else []) + (["dup", "dmid"] if mlp else []) + (["dqkv"] if att else [])
    ow = dict(dout=D, dup=FF, dmid=D, dqkv=saved["qkv"].shape[2] if att else 0)
    out_shape = [jax.ShapeDtypeStruct((NL, T, ow[n]), BF) for n in outs] + ([jax.ShapeDtypeStruct((T, D), BF)] if att else [])
    names = ["din_h"] + [n + "_h" for n in ins] + [n + "_h" for n in wn_h] + [n + "_h" for n in outs] + (["dfin_h"] if att else [])
    scratch = [("d", (R, D)), ("tmp", (R, D))] + [(n, (R, saved[n].shape[2])) for n in ins] + [(n, (3 * weights["wq"].shape[0], D) if n == "wqkv" else weights[n].shape) for n in wn] + [(n, (R, ow[n])) for n in outs] + [(n, (2, pu, LANE, 2 * LANE)) for n in ABUF if att]
    names += [n for n, _ in scratch] + ["wsem", "isem", "osem", "dsem", "fsem"]
    cfg = dict(R=R, NL=NL, lo=lo, mlp=mlp, att=att, ft=ft, pu=pu, ch=ch, nt=nt, names=names, weights=wn, ins=ins, outs=outs,
               c2=(64 ** -0.5) * math.log2(math.e), scale=64 ** -0.5, **kw)
    any_ = pl.BlockSpec(memory_space=pl.ANY)
    res = pl.pallas_call(
        functools.partial(bwd_kernel, cfg),
        grid=(T // R,),
        out_shape=out_shape,
        in_specs=[any_] * (1 + len(ins) + len(wn_h)),
        out_specs=[any_] * len(out_shape),
        scratch_shapes=[pltpu.VMEM(s, BF) for _, s in scratch] + [pltpu.SemaphoreType.DMA((8,))] + [pltpu.SemaphoreType.DMA((4,))] * 2 + [pltpu.SemaphoreType.DMA] * 2,
        compiler_params=pltpu.CompilerParams(vmem_limit_bytes=VLIM, dimension_semantics=("arbitrary",), flags=lp or {}),
        cost_estimate=pl.CostEstimate(flops=2 * NL * T * D * (2 * FF * mlp + 4 * D * att), bytes_accessed=2 * NL * T * (2 * FF * mlp + 8 * D), transcendentals=0),
        name="bwd_%d_%d%s%s" % (lo, NL, "m" if mlp else "", "a" if att else ""),
    )(din, *[saved[n] for n in ins], *[weights[n] for n in wn_h])
    return dict(zip(outs + (["dfin"] if att else []), res))


def wgrad_kernel(cfg, *refs):
    segs, RB, CU, lhs_res, sw = (cfg[k] for k in ("segs", "RB", "CU", "lhs_res", "sw"))
    ends = list(itertools.accumulate(n for _, _, n in segs))
    NU, P, rb2 = ends[-1], PARTS, 2 * RB
    res_h, str_h, pos = [], [], 0
    for na, nb, _ in segs:
        pair = refs[pos:pos + na], refs[pos + na:pos + na + nb]
        pos += na + nb
        res_h.append(pair[not lhs_res])
        str_h.append(pair[lhs_res])
    out, res, strip, acc, *rv = refs[pos:pos + 8]
    rsem, tsem, csem, ssem, qsem = refs[pos + 8:]
    cp = CU // P
    mb = min(2 * LANE, res.shape[1])
    rc = mb if lhs_res else 2 * mb
    nsub = NSUB
    me = lax.axis_index("data")
    bc = me % 2
    bits = [(me // 2 ** (d + 1)) % 2 for d in range(3)]
    core = me + 1 - 2 * bc

    def pick(be, vals):
        return jnp.where(be == 0, vals[0], jnp.where(be == 1, vals[1], vals[2]))

    def nbr(be):
        return me + pick(be, [(1 - 2 * bits[d]) * 2 ** (d + 1) for d in range(3)])

    def pieces(hs, dst, sem, cols):
        slabs = [h.at[q, :, cols] for h in hs for q in range(h.shape[0])]
        n = dst.shape[0] // len(slabs)
        return [pltpu.make_async_copy(h, dst.at[pl.ds(i * n, n)], sem) for i, h in enumerate(slabs)]

    def res_copies(k, j):
        return pieces(res_h[k], res.at[:, pl.ds(j * rc, rc)], rsem.at[j], pl.ds(j * rc, rc))

    def strip_copies(k, u):
        return pieces(str_h[k], strip.at[u % 2], tsem.at[u % 2], pl.ds(pl.multiple_of((u - (ends[k] - segs[k][2])) * sw, sw), sw))

    def start(cs):
        for c in cs:
            c.start()

    def wait(cs):
        for c in cs:
            c.wait()

    def start_strip(u):
        for k, e in enumerate(ends):
            pl.when((u >= e - segs[k][2]) & (u < e))(lambda: start(strip_copies(k, u)))

    start(strip_copies(0, 0))
    for j in range(res.shape[1] // rc):
        start(res_copies(0, j))
    bar = pltpu.get_barrier_semaphore()
    peers = [core] + [nbr(d) for d in range(3)]
    for t in peers:
        pl.semaphore_signal(bar, inc=1, device_id=(t,), device_id_type=pl.DeviceIdType.MESH)
    pl.semaphore_wait(bar, len(peers))

    def rcopy(src, dst, ss, rs, dev):
        return pltpu.make_async_remote_copy(src_ref=src, dst_ref=dst, send_sem=ss, recv_sem=rs, device_id=(dev,), device_id_type=pl.DeviceIdType.MESH)

    def core_copy(v, p):
        return rcopy(acc.at[v % 2, :, 1 - bc, :, pl.ds(p * cp, cp)], rv[0].at[v, p], csem.at[v % 2, p], qsem.at[0, v, p], core)

    def stage_copy(s, v, p):
        return rcopy(rv[0].at[v, p, pl.ds(0, BLOCKS >> s)], rv[s].at[v, p], ssem.at[s - 1, v, p], qsem.at[s, v, p], core)

    def stage(s, v):
        for p in range(P):
            order = [(v + p + d) % 3 for d in range(3)]
            wt = [pick(be, [2 ** d for d in range(3)]) for be in order]
            mine = [pick(be, bits) for be in order]
            held = [sum([mine[d] * wt[d] for d in range(s - (s > 0))], 0)]

            def blocks(lead, d0):
                for f in itertools.product(range(2), repeat=3 - d0):
                    yield lead + sum([b * w for b, w in zip(f, wt[d0:])], 0)
            cols = slice(p * cp, (p + 1) * cp)
            if s == 0:
                core_copy(v, p).wait_recv()
                for k in range(BLOCKS):
                    rv[0][v, p, k] += acc[v % 2, k, bc, :, cols]
            else:
                stage_copy(s, v, p).wait_recv()
                keep = held[0] + mine[s - 1] * wt[s - 1]
                for m, k in enumerate(blocks(keep, s)):
                    total = rv[0][v, p, k] + rv[s][v, p, m]
                    if s < 3:
                        rv[0][v, p, k] = total
                    elif lhs_res:
                        out[:, pl.ds(pl.multiple_of(v * CU + p * cp, LANE), cp)] = total
                    else:
                        out[v, :, cols] = total
                held[0] = keep
            if s < 3:
                for m, k in enumerate(blocks(held[0] + (1 - mine[s]) * wt[s], s + 1)):
                    rcopy(rv[0].at[v, p, k], rv[s + 1].at[v, p, m], ssem.at[s, v, p], qsem.at[s + 1, v, p], nbr(order[s])).start()

    def serve(s, v):
        pl.when((v >= 0) & (v < NU))(lambda: stage(s, v))

    def sub(u, i):
        mi, ni = (i, 0) if lhs_res else (i % 2, i // 2)
        j = mi if lhs_res else ni
        if lhs_res or mi == 0:
            for k, e in enumerate(ends):
                pl.when(u == e - segs[k][2])(lambda: wait(res_copies(k, j)))
        ms, ns, kk = slice(mi * mb, (mi + 1) * mb), slice(ni * sw, (ni + 1) * sw), mb // rb2
        lhs, rhs = (res[:, ms], strip[u % 2]) if lhs_res else (strip[u % 2, :, ms], res[:, ns])
        acc[u % 2, mi * kk:(mi + 1) * kk, :, :, ns] = dot(lhs, rhs, 0, 0).reshape(kk, 2, RB, sw)
        if i == 0:
            start_strip(u + 1)
        for k, e in enumerate(ends[:-1]):
            pl.when(u == e - 1)(lambda: start(res_copies(k + 1, j)))

    def unit(u, carry):
        live = u < NU

        @pl.when(live)
        def _():
            wait(pieces(str_h[0], strip.at[u % 2], tsem.at[u % 2], pl.ds(0, sw)))
            pl.when(u > 1)(lambda: [core_copy(u, p).wait_send() for p in range(P)] and None)
        for i in range(nsub):
            pl.when(live)(lambda: sub(u, i))
            for s, lag in SERVE[i]:
                serve(s, u - lag)
        pl.when(live)(lambda: [core_copy(u, p).start() for p in range(P)] and None)
        return carry
    lax.fori_loop(0, NU + SERVE[1][0][1], unit, 0)

    for v in range(max(0, NU - 2), NU):
        for p in range(P):
            core_copy(v, p).wait_send()

    def drain(v, carry):
        for p in range(P):
            for s in range(1, len(rv)):
                stage_copy(s, v, p).wait_send()
        return carry
    lax.fori_loop(0, NU, drain, 0)


def wgrad(segments, lhs_res, cid, name, sw=512):
    (a0, b0), K = segments[0], sum(a.shape[0] * a.shape[1] for a in segments[0][0])
    WA, WB = a0[0].shape[2], b0[0].shape[2]
    segs = [(len(a), len(b), (b if lhs_res else a)[0].shape[2] // sw) for a, b in segments]
    NU = sum(n for _, _, n in segs)
    WR, RU, CU = (WA, WA, sw) if lhs_res else (WB, sw, WB)
    RB, cp = RU // DEVS, CU // PARTS
    out_sd = jax.ShapeDtypeStruct((RB, NU * sw) if lhs_res else (NU, RB, CU), F32)
    any_ = pl.BlockSpec(memory_space=pl.ANY)
    dma = pltpu.SemaphoreType.DMA
    ops = [x for a, b in segments for x in (*a, *b)]
    return pl.pallas_call(
        functools.partial(wgrad_kernel, dict(segs=segs, RB=RB, CU=CU, lhs_res=lhs_res, sw=sw)),
        out_shape=out_sd,
        in_specs=[any_] * len(ops),
        out_specs=pl.BlockSpec(memory_space=pltpu.VMEM),
        scratch_shapes=[pltpu.VMEM((K, WR), BF), pltpu.VMEM((2, K, sw), BF), pltpu.VMEM((2, BLOCKS, 2, RB, CU), F32)]
        + [pltpu.VMEM((NU, PARTS, BLOCKS >> s, RB, cp), F32) for s in range(NSUB)]
        + [dma((NSUB,)), dma((2,)), dma((2, PARTS)), dma((NSUB - 1, NU, PARTS)), dma((NSUB, NU, PARTS))],
        compiler_params=pltpu.CompilerParams(vmem_limit_bytes=VLIM, collective_id=cid, has_side_effects=True),
        cost_estimate=pl.CostEstimate(flops=2 * K * RU * CU * NU, bytes_accessed=2 * K * (WA + WB), transcendentals=0),
        name=name,
    )(*ops)


def copy_kernel(plan, *refs):
    n = len(plan)
    srcs, dsts, (buf, isem, osem) = refs[:n], refs[n:2 * n], refs[2 * n:]
    depth, rows, width = buf.shape
    jobs = []
    for (r0, c0), src, dst in zip(plan, srcs, dsts):
        for c in range(0, dst.shape[1], width):
            jobs += [(src.at[pl.ds(r0 + r, rows), pl.ds(c0 + c, width)], dst.at[pl.ds(r, rows), pl.ds(c, width)]) for r in range(0, dst.shape[0], rows)]

    def cin(i):
        return pltpu.make_async_copy(jobs[i][0], buf.at[i % depth], isem.at[i % depth])

    def cout(i):
        return pltpu.make_async_copy(buf.at[i % depth], jobs[i][1], osem.at[i % depth])
    ahead = depth // 2
    for i in range(min(ahead, len(jobs))):
        cin(i).start()
    for i in range(len(jobs)):
        j = i + ahead
        if j < len(jobs):
            if j >= depth:
                cout(j - depth).wait()
            cin(j).start()
        cin(i).wait()
        cout(i).start()
    for i in range(max(0, len(jobs) - depth), len(jobs)):
        cout(i).wait()


def copy_out(parts, n_rows=None, rows=512, depth=16):
    any_ = pl.BlockSpec(memory_space=pl.ANY)
    outs = [jax.ShapeDtypeStruct((n_rows or a.shape[0], w), F32) for a, _, _, w in parts]
    dma = pltpu.SemaphoreType.DMA((depth,))
    size = sum(o.size for o in outs)
    return pl.pallas_call(
        functools.partial(copy_kernel, [(r, c) for _, r, c, _ in parts]),
        out_shape=outs,
        in_specs=[any_] * len(parts),
        out_specs=[any_] * len(parts),
        scratch_shapes=[pltpu.VMEM((depth, rows, min(o.shape[1] for o in outs)), F32), dma, dma],
        compiler_params=pltpu.CompilerParams(vmem_limit_bytes=VLIM),
        cost_estimate=pl.CostEstimate(flops=size * rows, bytes_accessed=2 * size, transcendentals=0),
        name="copy_out",
    )(*[a for a, _, _, _ in parts])


def solution(mesh):
    batch_spec = P('data', None, None)

    def per_device(x_loc, g_loc, step_emb, w_q, w_k, w_v, w_o, w_up, w_down):
        n_seq, seq, d = x_loc.shape
        heads, hd = w_q.shape[1], w_q.shape[2]
        qw = heads * hd
        t = n_seq * seq
        flat_t = [w.transpose(1, 2, 0).reshape(qw, d) for w in (w_q, w_k, w_v)]
        weights = dict(wq=flat_t[0], wk=flat_t[1], wv=flat_t[2], wo=w_o.reshape(qw, d), wup=w_up, wdown=w_down)
        n_layers = step_emb.shape[0]
        xs, us, qkv, mix, hs, ms, z, g = fwd(x_loc.reshape(t, d), step_emb, *flat_t, weights["wo"], w_up, w_down)
        saved = dict(xs=xs, qkv=qkv, hs=hs, z=z)
        top = bwd(g_loc.reshape(t, d), saved, weights, n_layers - 1, 1)
        d0 = top["dfin"]
        down = wgrad([([g], [d0[None], top["dout"]])], False, 1, "wgrad_down")
        d0, down = lax.optimization_barrier((d0, down))
        ag_down = lax.all_gather(down, 'data', axis=1, tiled=True)
        low = bwd(d0, saved, weights, 1, 0, att=False)
        dmid0 = low["dmid"]
        upo = wgrad([([ms], [low["dup"], top["dup"]]), ([mix], [dmid0, top["dmid"]])], True, 2, "wgrad_up_o")
        dmid0, upo, ag_down = lax.optimization_barrier((dmid0, upo, ag_down))
        ag_upo = lax.all_gather(upo, 'data', axis=0, tiled=True)
        bot = bwd(dmid0[0], saved, weights, 1, 0, mlp=False)
        gqkv = wgrad([([bot["dqkv"], top["dqkv"]], [us])], False, 3, "wgrad_qkv")
        gqkv, ag_upo = lax.optimization_barrier((gqkv, ag_upo))
        ag_qkv = lax.all_gather(gqkv, 'data', axis=1, tiled=True)
        ff = w_up.shape[1]
        gup, go, gdown = copy_out([(ag_upo, 0, 0, ff), (ag_upo, 0, ff, d), (ag_down.reshape(w_down.shape), 0, 0, d)])
        flat = ag_qkv.reshape(3 * qw, d)
        gq, gk, gv = (w.reshape(heads, hd, d).transpose(2, 0, 1) for w in copy_out([(flat, i * qw, 0, d) for i in range(3)], qw))
        return (gq, gk, gv, go.reshape(heads, hd, d), gup, gdown, bot["dfin"].reshape(x_loc.shape))

    return jax.shard_map(per_device, mesh=mesh, in_specs=(batch_spec, batch_spec, P(), P(), P(), P(), P(), P(), P()), out_specs=(P(), P(), P(), P(), P(), P(), batch_spec), check_vma=False)
```
